32 devices in a mesh: dp: 8 (over z, x), expert: 4 (over y, core).
Axes of the slice: x: 2, y: 2, z: 4, core: 2. Of those that a mesh axis runs over, the one named last changes fastest.
Arguments:
- tokens: bfloat16 [4096, 4096], P(('dp', 'expert')), may hold values from -6 to 6
- select: int32 [4, 128], P(None, ('dp', 'expert')), may hold values from -1 to 127, as said below
- gates: float32 [4, 128], P(None, ('dp', 'expert')), may hold values from 0.1 to 1
- w_gate: bfloat16 [4, 4096, 8192], P('expert', None, 'dp'), may hold values from -0.09375 to 0.09375
- w_up: bfloat16 [4, 4096, 8192], P('expert', None, 'dp'), may hold values from -0.09375 to 0.09375
- w_down: bfloat16 [4, 8192, 4096], P('expert', 'dp'), may hold values from -0.0625 to 0.0625
Outputs:
- mixed: bfloat16 [4096, 4096], P(('dp', 'expert'))
The draws below stay inside these ranges and needn't reach their ends.
Inputs may be any that keep to these rules, and one draw needn't show every extreme that they name: `select`: in each block of 4 slots of a row, the live entries come first, distinct and ascending, below 128, followed by -1; every block holds at least one live entry, and every expert fills all 4 slots of some source device.
All inputs are finite; a program needn't handle non-finite values.
Results may differ from the reference program's by a relative error of at most 0.0085.
Values may be sent and summed in bfloat16 or wider, within the bound.
No kernel may reach another device: no remote copies, remote signals or barrier semaphores. Data moves between devices by JAX's collectives and lax.ppermute only.
A program may use at most 64 MiB of HBM per device.

```python
import jax
import jax.numpy as jnp

D = 4096
FF = 8192
TOK_DEV = 128
EXPERTS = 4
SLOT = 4
TOKENS = 4096
DEVICES = 32


def draw_select(key, part):
    keys_all = jax.random.split(jax.random.fold_in(key, 11), EXPERTS * DEVICES)

    def one_block(sub_key):
        chosen = jax.random.permutation(sub_key, TOK_DEV)[:SLOT]
        return jnp.sort(chosen)
    picks = jax.vmap(one_block)(keys_all).reshape(EXPERTS, DEVICES, SLOT)
    counts = jax.random.randint(jax.random.fold_in(key, 7), (EXPERTS, DEVICES), 1, SLOT + 1)
    full_src = (jnp.arange(EXPERTS)[:, None] * 37 + 3) % DEVICES
    counts = jnp.where(jnp.arange(DEVICES)[None, :] == full_src, SLOT, counts)
    slot_pos = jnp.arange(SLOT)
    result = jnp.where(slot_pos[None, None, :] < counts[:, :, None], picks, -1)
    return result.reshape(EXPERTS, DEVICES * SLOT).astype(jnp.int32)


def steps_of(key, dims, cuts, least, top_value):
    def one(axis_at, shards_of):
        draws = jax.random.uniform(jax.random.fold_in(jax.random.fold_in(key, 6), axis_at), (shards_of,), jnp.float32, least / len(cuts), top_value / len(cuts))
        return jnp.repeat(jnp.exp(draws), dims[axis_at] // shards_of).reshape((-1,) + (1,) * (len(dims) - axis_at - 1))

    level = one(*cuts[0])
    for cut in cuts[1:]:
        level = level * one(*cut)
    return level


def bell_draw(own_key, extent, scale, bound, pieces=(), held_as=jnp.bfloat16):
    values = jax.random.normal(own_key, extent, jnp.float32) * scale
    if len(pieces) > 0:
        values = steps_of(own_key, extent, pieces, -0.22, 0.18) * values
    return jnp.clip(values, min=-bound, max=bound).astype(held_as)


def setup_inputs(seed: int = 0) -> dict:
    key_of = jax.random.split(jax.random.key(seed), 7)
    tokens = bell_draw(key_of[0], (TOKENS, D), 1.0, 6.0, ((0, 32),))
    select = draw_select(jax.random.fold_in(key_of[6], 71), 0)
    gates = jnp.clip(0.1 + 0.9 * jax.random.uniform(key_of[2], (EXPERTS, DEVICES * SLOT), jnp.float32) ** steps_of(key_of[2], (EXPERTS, DEVICES * SLOT), ((1, 32),), -0.2, 0.2), 0.1, 1.0)
    w_gate = bell_draw(key_of[3], (EXPERTS, D, FF), D ** -0.5, 0.09375, ((0, 4), (2, 8)))
    w_up = bell_draw(key_of[4], (EXPERTS, D, FF), D ** -0.5, 0.09375, ((0, 4), (2, 8)))
    w_down = bell_draw(key_of[5], (EXPERTS, FF, D), FF ** -0.5, 0.0625, ((0, 4), (1, 8)))
    return {"tokens": tokens, "select": select, "gates": gates, "w_gate": w_gate, "w_up": w_up, "w_down": w_down}


def reference(tokens, select, gates, w_gate, w_up, w_down):
    mixed = jnp.zeros((TOKENS, D), jnp.float32)
    source = (jnp.arange(DEVICES * SLOT) // SLOT).astype(jnp.int32)
    for expert_id in range(EXPERTS):
        index_row = select[expert_id]
        is_live = index_row >= 0
        global_idx = (source * TOK_DEV + jnp.where(is_live, index_row, 0)).astype(jnp.int32)
        sel_rows = jnp.where(is_live[:, None], tokens[global_idx], 0).astype(jnp.bfloat16)
        gate_val = jnp.dot(sel_rows, w_gate[expert_id], preferred_element_type=jnp.float32)
        up_val = jnp.dot(sel_rows, w_up[expert_id], preferred_element_type=jnp.float32)
        hidden = (jax.nn.silu(gate_val) * up_val).astype(jnp.bfloat16)
        expert_out = jnp.dot(hidden, w_down[expert_id], preferred_element_type=jnp.float32).astype(jnp.bfloat16)
        weight_col = jnp.where(is_live, gates[expert_id], 0.0).astype(jnp.float32)
        mixed = mixed.at[global_idx].add(weight_col[:, None] * expert_out.astype(jnp.float32))
    return mixed.astype(jnp.bfloat16)
```

```python
import jax
import jax.numpy as jnp
from jax import lax
from jax.sharding import PartitionSpec as P


def swap(value, axis_name, size, mask):
    if mask == 0:
        return value
    return lax.ppermute(value, axis_name, [(i, i ^ mask) for i in range(size)])


def expert_ffn(rows, w_gate, w_up, w_down):
    gate_val = jnp.dot(rows, w_gate, preferred_element_type=jnp.float32)
    up_val = jnp.dot(rows, w_up, preferred_element_type=jnp.float32)
    hidden = (jax.nn.silu(gate_val) * up_val).astype(jnp.bfloat16)
    return jnp.dot(hidden, w_down, preferred_element_type=jnp.float32)


def gather_two_level(value, axis_name, size, inner):
    half = value.shape[1] // 2
    inner_masks = range(inner)
    outer_masks = range(0, size, inner)

    def stage(v, masks):
        return [swap(v, axis_name, size, m) for m in masks]

    left = jnp.concatenate(stage(value[:, :half], inner_masks), 0)
    left = jnp.concatenate(stage(left, outer_masks), 0)
    right = stage(value[:, half:], outer_masks)
    right = stage(jnp.concatenate(right, 0), inner_masks)
    n = value.shape[0]
    blocks = [right[m % inner][(m // inner) * n:(m // inner + 1) * n] for m in range(size)]
    return jnp.concatenate([left, jnp.concatenate(blocks, 0)], 1)


def solution(mesh):
    n_dp = mesh.shape["dp"]
    n_exp = mesh.shape["expert"]
    inner = 1
    while inner * inner * 4 <= n_dp:
        inner *= 2

    def per_device(tokens, select, gates, w_gate, w_up, w_down):
        experts, slot_count = select.shape
        tok_dev, width = tokens.shape
        order = lax.axis_index("expert") ^ jnp.arange(experts, dtype=jnp.int32)
        picks = jnp.take(select, order, axis=0).reshape(-1)
        weights = jnp.take(gates, order, axis=0).reshape(-1)
        is_live = picks >= 0
        safe_idx = jnp.where(is_live, picks, 0)
        sel_rows = jnp.where(is_live[:, None], jnp.take(tokens, safe_idx, axis=0), 0)
        arrived = jnp.concatenate(
            [swap(sel_rows[k * slot_count:(k + 1) * slot_count], "expert", n_exp, k) for k in range(n_exp)], 0)
        rows = gather_two_level(arrived, "dp", n_dp, inner)
        partial = expert_ffn(rows, w_gate[0], w_up[0], w_down[0]).astype(jnp.bfloat16)
        n = experts * slot_count
        summed = partial[:n].astype(jnp.float32)
        for m in range(1, n_dp):
            summed = summed + swap(partial[m * n:(m + 1) * n], "dp", n_dp, m).astype(jnp.float32)
        summed = summed.astype(jnp.bfloat16)
        returned = jnp.concatenate(
            [swap(summed[k * slot_count:(k + 1) * slot_count], "expert", n_exp, k) for k in range(n_exp)], 0)
        token_ids = jnp.arange(tok_dev, dtype=jnp.int32)
        combine = jnp.where((picks[None, :] == token_ids[:, None]), weights[None, :], 0.0)
        mixed = jnp.dot(combine, returned.astype(jnp.float32), precision=lax.Precision.HIGHEST)
        return mixed.astype(jnp.bfloat16)

    return jax.shard_map(
        per_device,
        mesh=mesh,
        in_specs=(
            P(("dp", "expert"), None),
            P(None, ("dp", "expert")),
            P(None, ("dp", "expert")),
            P("expert", None, "dp"),
            P("expert", None, "dp"),
            P("expert", "dp", None),
        ),
        out_specs=P(("dp", "expert"), None),
        check_vma=False,
    )
```

```python
import jax
import jax.numpy as jnp
from jax import lax
from jax.experimental import pallas as pl
from jax.experimental.pallas import tpu as pltpu
from jax.sharding import PartitionSpec as P


def swap(value, axis_name, size, mask):
    if mask == 0:
        return value
    return lax.ppermute(value, axis_name, [(i, i ^ mask) for i in range(size)])


def expert_ffn(pieces, w_gate, w_up, w_down):
    count = len(pieces)
    n, width = pieces[0].shape
    hidden_units = w_gate.shape[1]
    step = min(512, hidden_units)
    out_step = min(1024, width)
    n_in, n_out = hidden_units // step, width // out_step

    def body(*refs):
        row_in, (g_hbm, u_hbm, d_hbm) = refs[:count], refs[count:count + 3]
        outs = refs[count + 3:2 * count + 3]
        r_ref, g_ref, u_ref, d_ref, h_ref, row_sems, g_sems, u_sems, d_sems = refs[2 * count + 3:]

        def start(src, dst, sem):
            copy = pltpu.make_async_copy(src, dst, sem)
            copy.start()
            return copy

        rows = [start(row_in[k], r_ref.at[k * n:(k + 1) * n], row_sems.at[k]) for k in range(count)]
        ins = []
        for j in range(n_in):
            cols = slice(j * step, (j + 1) * step)
            ins.append((start(g_hbm.at[:, cols], g_ref.at[:, cols], g_sems.at[j]),
                        start(u_hbm.at[:, cols], u_ref.at[:, cols], u_sems.at[j])))
        downs = []
        for j in range(n_out):
            cols = slice(j * out_step, (j + 1) * out_step)
            downs.append(start(d_hbm.at[:, cols], d_ref.at[:, cols], d_sems.at[j]))
        for c in rows:
            c.wait()
        for j in range(n_in):
            cols = slice(j * step, (j + 1) * step)
            ins[j][0].wait()
            gate_val = jnp.dot(r_ref[...], g_ref[:, cols], preferred_element_type=jnp.float32)
            ins[j][1].wait()
            up_val = jnp.dot(r_ref[...], u_ref[:, cols], preferred_element_type=jnp.float32)
            h_ref[:, cols] = (gate_val / (1.0 + jnp.exp(-gate_val)) * up_val).astype(jnp.bfloat16)
        for j in range(n_out):
            cols = slice(j * out_step, (j + 1) * out_step)
            downs[j].wait()
            part = jnp.dot(h_ref[...], d_ref[:, cols], preferred_element_type=jnp.float32).astype(jnp.bfloat16)
            for k in range(count):
                outs[k][:, cols] = part[k * n:(k + 1) * n]

    hbm = pl.BlockSpec(memory_space=pl.ANY)
    vm = pl.BlockSpec(memory_space=pltpu.VMEM)
    total = count * n
    weight_bytes = 2 * (w_gate.size + w_up.size + w_down.size)
    return pl.pallas_call(
        body,
        out_shape=[jax.ShapeDtypeStruct((n, width), jnp.bfloat16)] * count,
        in_specs=[hbm] * (count + 3),
        out_specs=[vm] * count,
        scratch_shapes=[
            pltpu.VMEM((total, width), jnp.bfloat16),
            pltpu.VMEM(w_gate.shape, w_gate.dtype),
            pltpu.VMEM(w_up.shape, w_up.dtype),
            pltpu.VMEM(w_down.shape, w_down.dtype),
            pltpu.VMEM((total, hidden_units), jnp.bfloat16),
            pltpu.SemaphoreType.DMA((count,)),
            pltpu.SemaphoreType.DMA((n_in,)),
            pltpu.SemaphoreType.DMA((n_in,)),
            pltpu.SemaphoreType.DMA((n_out,)),
        ],
        cost_estimate=pl.CostEstimate(
            flops=total * weight_bytes, transcendentals=total * hidden_units, bytes_accessed=weight_bytes),
        name="expert_ffn",
    )(*pieces, w_gate, w_up, w_down)


def spread(value, axis_name, size, masks):
    return [value] + [swap(value, axis_name, size, m) for m in masks]


def collect(pieces, axis_name, size, masks):
    total = pieces[0].astype(jnp.float32)
    for piece, m in zip(pieces[1:], masks):
        total = total + swap(piece, axis_name, size, m).astype(jnp.float32)
    return total.astype(jnp.bfloat16)


def solution(mesh):
    n_dp = mesh.shape["dp"]
    n_exp = mesh.shape["expert"]
    near = min(4, n_dp)
    both = ("dp", "expert")
    far_masks = [m * near for m in range(n_dp // near)]
    near_masks = list(range(1, near))

    def per_device(tokens, select, gates, w_gate, w_up, w_down):
        experts, slot_count = select.shape
        tok_dev, width = tokens.shape
        order = lax.axis_index("expert") ^ jnp.arange(experts, dtype=jnp.int32)
        picks = jnp.take(select, order, axis=0).reshape(-1)
        weights = jnp.take(gates, order, axis=0).reshape(-1)
        is_live = picks >= 0
        safe_idx = jnp.where(is_live, picks, 0)
        sel_rows = jnp.where(is_live[:, None], jnp.take(tokens, safe_idx, axis=0), 0)
        slots = [sel_rows[k * slot_count:(k + 1) * slot_count] for k in range(experts)]
        held = jnp.concatenate(
            [swap(slots[k], both, n_dp * n_exp, m * n_exp + k) for m in far_masks for k in range(experts)], 0)
        pieces = spread(held, "dp", n_dp, near_masks)
        partial = expert_ffn(pieces, w_gate[0], w_up[0], w_down[0])
        near_sum = collect(partial, "dp", n_dp, near_masks)
        blocks = near_sum.reshape(len(far_masks), experts, slot_count, width)
        returned = 0.0
        for i, m in enumerate(far_masks):
            back = [swap(blocks[i, k], both, n_dp * n_exp, m * n_exp + k) for k in range(experts)]
            returned = returned + jnp.concatenate(back, 0).astype(jnp.float32)
        token_ids = jnp.arange(tok_dev, dtype=jnp.int32)
        combine = jnp.where((picks[None, :] == token_ids[:, None]), weights[None, :], 0.0)
        mixed = jnp.dot(combine, returned, precision=lax.Precision.HIGHEST)
        return mixed.astype(jnp.bfloat16)

    return jax.shard_map(
        per_device,
        mesh=mesh,
        in_specs=(
            P(("dp", "expert"), None),
            P(None, ("dp", "expert")),
            P(None, ("dp", "expert")),
            P("expert", None, "dp"),
            P("expert", None, "dp"),
            P("expert", "dp", None),
        ),
        out_specs=P(("dp", "expert"), None),
        check_vma=False,
    )
```
